32 devices in a mesh: ang: 8 (over y, x, core), img: 4 (over z).
Axes of the slice: x: 2, y: 2, z: 4, core: 2. Of those that a mesh axis runs over, the one named last changes fastest.
Arguments:
- sinogram: bfloat16 [16, 64, 4096], P('ang', None, 'img'), may hold values from -4 to 28
- offsets: int32 [16], replicated, may hold values from 0 to 65504, as said below
- steps: int32 [16, 2], replicated, may hold values from -32 to 32, as said below
Outputs:
- picture: bfloat16 [1024, 64, 1024], P('ang', None, 'img')
The draws below stay inside these ranges and needn't reach their ends.
Inputs may be any that keep to these rules, and one draw needn't show every extreme that they name: Each row (u, v) of steps satisfies u^2 + v^2 <= 32^2 < (|u| + 1)^2 + (|v| + 1)^2. For every angle a and every pixel (y, x) with 0 <= x, y < 1024, offsets[a] + steps[a, 0] x + steps[a, 1] y lies in 0 to 65504.
All inputs are finite; a program needn't handle non-finite values.
Results may differ from the reference program's by a relative error of at most 0.0053.
Values may be sent and summed in bfloat16 or wider, within the bound.
No kernel may reach another device: no remote copies, remote signals or barrier semaphores. Data moves between devices by JAX's collectives and lax.ppermute only.
A program may use at most 192 MiB of HBM per device.

```python
import math
import jax
import jax.numpy as jnp
from jax import lax

BINS = 4096
IMG = 1024
SLICES = 64
ANGLES = 16
STEP_MAX = 32


def lattice_steps(key):
    base_key = jax.random.fold_in(key, 5417)
    key_first, key_sign, key_swap = jax.random.split(base_key, 3)
    first_part = jax.random.randint(key_first, (ANGLES,), -STEP_MAX, STEP_MAX + 1, dtype=jnp.int32)
    remains = STEP_MAX * STEP_MAX - first_part * first_part
    counter = jnp.arange(1, STEP_MAX + 1, dtype=jnp.int32)
    magnitude = jnp.sum((counter[None, :] * counter[None, :] <= remains[:, None]).astype(jnp.int32), axis=1).astype(jnp.int32)
    sign_value = jax.random.randint(key_sign, (ANGLES,), 0, 2, dtype=jnp.int32) * 2 - 1
    second_part = sign_value * magnitude
    swapped = jax.random.randint(key_swap, (ANGLES,), 0, 2, dtype=jnp.int32) == 1
    along_x = jnp.where(swapped, second_part, first_part)
    along_y = jnp.where(swapped, first_part, second_part)
    angle_order = jnp.arange(ANGLES, dtype=jnp.int32)
    along_x = jnp.where(angle_order == 0, -jnp.abs(along_x), jnp.where(angle_order == 1, jnp.abs(along_x), along_x))
    along_y = jnp.where(angle_order == 0, -jnp.abs(along_y), jnp.where(angle_order == 1, jnp.abs(along_y), along_y))
    return jnp.stack([along_x, along_y], axis=1).astype(jnp.int32)


def geometry(key):
    step_pairs = lattice_steps(key)
    key_room = jax.random.fold_in(key, 7321)
    spread = (IMG - 1) * (jnp.abs(step_pairs[:, 0]) + jnp.abs(step_pairs[:, 1]))
    spare_room = 16 * (BINS - 2) - spread
    shift_in = jax.random.randint(key_room, (ANGLES,), 0, spare_room + 1, dtype=jnp.int32)
    angle_order = jnp.arange(ANGLES, dtype=jnp.int32)
    shift_in = jnp.where(angle_order == 0, spare_room, jnp.where(angle_order == 1, 0, shift_in))
    anchor = shift_in - (IMG - 1) * (jnp.minimum(step_pairs[:, 0], 0) + jnp.minimum(step_pairs[:, 1], 0))
    return (anchor.astype(jnp.int32), step_pairs)


def draw_offsets(key, part):
    return geometry(key)[0]


def draw_steps(key, part):
    return geometry(key)[1]


def bump_profile(bins_axis, center, half_width, height):
    ratio = (bins_axis - center) / half_width
    return height * jnp.sqrt(jnp.maximum(1.0 - ratio * ratio, 0.0))


def draw_sinogram(key, part):
    base_key = jax.random.fold_in(key, 911)
    key_list = jax.random.split(base_key, 16)
    row_shape = (ANGLES, SLICES, 1)
    bins_axis = jnp.arange(BINS, dtype=jnp.float32)[None, None, :]
    rough_part = jnp.clip(jax.random.normal(key_list[1], (ANGLES, SLICES, BINS), jnp.float32), -4.0, 4.0)
    body_low, body_high = (3.0, 6.0)
    small_low, small_high = (1.5, 4.0)
    summed = rough_part
    body_half = BINS * jax.random.uniform(key_list[2], row_shape, jnp.float32, 0.25, 0.45)
    body_center = body_half + jax.random.uniform(key_list[3], row_shape, jnp.float32) * (BINS - 2.0 * body_half)
    body_height = jax.random.uniform(key_list[4], row_shape, jnp.float32, body_low, body_high)
    summed = summed + bump_profile(bins_axis, body_center, body_half, body_height)
    for which in range(3):
        half_width = BINS * jnp.exp(jax.random.uniform(key_list[5 + 3 * which], row_shape, jnp.float32, math.log(1.0 / 16.0), math.log(0.25)))
        center = half_width + jax.random.uniform(key_list[6 + 3 * which], row_shape, jnp.float32) * (BINS - 2.0 * half_width)
        height = jax.random.uniform(key_list[7 + 3 * which], row_shape, jnp.float32, small_low, small_high)
        summed = summed + bump_profile(bins_axis, center, half_width, height)
    return summed.astype(jnp.bfloat16)


def setup_inputs(seed: int = 0) -> dict:
    streams_of = jax.random.split(jax.random.key(seed), 4)
    sinogram = draw_sinogram(jax.random.fold_in(streams_of[3], 71), 0)
    offsets = draw_offsets(jax.random.fold_in(streams_of[3], 71), 0)
    steps = draw_steps(jax.random.fold_in(streams_of[3], 71), 0)
    return dict(sinogram=sinogram, offsets=offsets, steps=steps)


def ramp_table():
    bin_index = jnp.arange(BINS, dtype=jnp.int32)
    offset_gap = bin_index[None, :] - bin_index[:, None]
    safe_gap = jnp.where(offset_gap == 0, 1, offset_gap).astype(jnp.float32)
    odd_gap = offset_gap % 2 != 0
    kernel = jnp.where(offset_gap == 0, jnp.float32(0.25), jnp.where(odd_gap, -1.0 / (math.pi ** 2 * safe_gap * safe_gap), jnp.float32(0.0)))
    return kernel.astype(jnp.float32)

def reference(sinogram, offsets, steps):
    ramp_rows = ramp_table()
    filtered = jnp.dot(sinogram.reshape(-1, BINS).astype(jnp.float32), ramp_rows, precision=lax.Precision.HIGHEST, preferred_element_type=jnp.float32)
    filtered = filtered.astype(jnp.bfloat16).reshape(sinogram.shape)
    rows_iota = jnp.arange(IMG, dtype=jnp.int32)
    cols_iota = jnp.arange(IMG, dtype=jnp.int32)

    def one_angle(summed, angle_data):
        filtered_one, offset, step_pair = angle_data
        position = offset + step_pair[0] * cols_iota[None, :] + step_pair[1] * rows_iota[:, None]
        low_bin = (position // 16).astype(jnp.int32)
        upper_weight = (position % 16).astype(jnp.float32) / 16.0
        values = filtered_one.astype(jnp.float32)
        lower_val = jnp.take(values, low_bin.reshape(-1), axis=1).reshape(SLICES, IMG, IMG)
        upper_val = jnp.take(values, (low_bin + 1).reshape(-1), axis=1).reshape(SLICES, IMG, IMG)
        contrib = (1.0 - upper_weight)[None] * lower_val + upper_weight[None] * upper_val
        return (summed + jnp.transpose(contrib, (1, 0, 2)), None)
    start_sum = jnp.zeros((IMG, SLICES, IMG), jnp.float32)
    summed = lax.scan(one_angle, start_sum, (filtered, offsets, steps))[0]
    return (summed * (2.0 / math.sqrt(ANGLES))).astype(jnp.bfloat16)
```

```python
import functools
import math

import jax
import jax.numpy as jnp
from jax import lax
from jax.experimental import pallas as pl
from jax.experimental.pallas import tpu as pltpu
from jax.sharding import PartitionSpec as P

IMG = 1024
STEP_MAX = 32
TILE = 16
BLOCK = 256
LANES = 128
REACH = math.isqrt(2 * STEP_MAX * STEP_MAX)
BAND = -(-(((TILE - 1) * REACH + TILE - 1) // TILE + 2) // 16) * 16


def window_rows(tiles_across, tiles_down):
    far = math.isqrt(STEP_MAX**2 * ((tiles_across - 1) ** 2 + (tiles_down - 1) ** 2))
    return -(-(far + BAND) // 16) * 16


def tile_floor(off, u, v):
    return (off + (TILE - 1) * (jnp.minimum(u, 0) + jnp.minimum(v, 0))) >> 4


def low_corner(u, v, tiles_across, tiles_down):
    return jnp.minimum(u, 0) * (tiles_across - 1) + jnp.minimum(v, 0) * (tiles_down - 1)


def ramp_kernel(bins, hi_ref, lo_ref):
    step = pl.program_id(0)
    shape = hi_ref.shape
    row = lax.broadcasted_iota(jnp.int32, shape, 0)
    col = lax.broadcasted_iota(jnp.int32, shape, 1)
    gap = col - row + (bins - BLOCK) - step * BLOCK
    safe = jnp.where(gap == 0, 1, gap).astype(jnp.float32)
    tail = jnp.where((gap & 1) != 0, -1.0 / (math.pi**2 * safe * safe), 0.0)
    value = jnp.where(gap == 0, 0.25, tail)
    hi = value.astype(jnp.bfloat16)
    hi_ref[...] = hi
    lo_ref[...] = (value - hi.astype(jnp.float32)).astype(jnp.bfloat16)


def ramp_strip(bins):
    blocks = 2 * bins // BLOCK - 1
    mid = bins // BLOCK - 2
    return pl.pallas_call(
        functools.partial(ramp_kernel, bins),
        grid=(blocks,),
        out_specs=[
            pl.BlockSpec((BLOCK, BLOCK), lambda k: (k, 0)),
            pl.BlockSpec((BLOCK, BLOCK), lambda k: (jnp.clip(k - mid, 0, 2), 0)),
        ],
        out_shape=[
            jax.ShapeDtypeStruct((blocks * BLOCK, BLOCK), jnp.bfloat16),
            jax.ShapeDtypeStruct((3 * BLOCK, BLOCK), jnp.bfloat16),
        ],
        cost_estimate=pl.CostEstimate(
            flops=20 * blocks * BLOCK * BLOCK, bytes_accessed=2 * blocks * BLOCK * BLOCK, transcendentals=0
        ),
        name="ramp_strip",
    )()


def filter_kernel(
    targets, tiles_across, tiles_down, win, off_ref, step_ref, hi_ref, lo_ref, x_ref, out_ref, xs_ref, ft_ref
):
    pieces, rows, piece_bins = x_ref.shape
    bins = pieces * piece_bins
    blocks = bins // BLOCK
    edge = jnp.zeros((rows, BLOCK), jnp.bfloat16)
    xs_ref[:, 0:BLOCK] = edge
    xs_ref[:, BLOCK + bins :] = edge
    for q in range(pieces):
        xs_ref[:, BLOCK + q * piece_bins : BLOCK + (q + 1) * piece_bins] = x_ref[q]
    ft_ref[bins:, :] = jnp.zeros((ft_ref.shape[0] - bins, LANES), jnp.float32)

    def one_block(kb, carry):
        start = pl.multiple_of((blocks - 1 - kb) * BLOCK, BLOCK)
        here = pl.multiple_of(kb * BLOCK, BLOCK)
        total = jnp.dot(
            xs_ref[:, BLOCK : BLOCK + bins], hi_ref[pl.ds(start, bins), :], preferred_element_type=jnp.float32
        )
        total += jnp.dot(xs_ref[:, pl.ds(here, 3 * BLOCK)], lo_ref[...], preferred_element_type=jnp.float32)
        for half in range(BLOCK // LANES):
            ft_ref[pl.ds(here + half * LANES, LANES), :] = total[:, half * LANES : (half + 1) * LANES].T
        return carry

    lax.fori_loop(0, blocks, one_block, 0, unroll=2)

    first = lax.axis_index("ang") * 2
    column = lax.axis_index("img")
    lane = lax.broadcasted_iota(jnp.int32, (win, LANES), 1)

    def one_target(t, carry):
        start = []
        for k in range(2):
            u, v = step_ref[first + k, 0], step_ref[first + k, 1]
            start.append(
                tile_floor(off_ref[first + k], u, v)
                + u * (column * tiles_across)
                + v * (t * tiles_down)
                + low_corner(u, v, tiles_across, tiles_down)
            )
        both = jnp.where(lane < LANES // 2, ft_ref[pl.ds(start[0], win), :], ft_ref[pl.ds(start[1], win), :])
        out_ref[t] = both.astype(jnp.bfloat16)
        return carry

    lax.fori_loop(0, targets, one_target, 0)


def filter_windows(pieces, offsets, steps, targets, tiles_across, tiles_down):
    count, rows, piece_bins = pieces.shape
    bins = count * piece_bins
    win = window_rows(tiles_across, tiles_down)
    hi, lo = ramp_strip(bins)
    vmem = pl.BlockSpec(memory_space=pltpu.VMEM)
    smem = pl.BlockSpec(memory_space=pltpu.SMEM)
    return pl.pallas_call(
        functools.partial(filter_kernel, targets, tiles_across, tiles_down, win),
        in_specs=[smem, smem, vmem, vmem, vmem],
        out_specs=vmem,
        out_shape=jax.ShapeDtypeStruct((targets, win, LANES), jnp.bfloat16),
        scratch_shapes=[
            pltpu.VMEM((rows, bins + 2 * BLOCK), jnp.bfloat16),
            pltpu.VMEM((bins + win, LANES), jnp.float32),
        ],
        compiler_params=pltpu.CompilerParams(vmem_limit_bytes=40 * 1024 * 1024),
        cost_estimate=pl.CostEstimate(
            flops=2 * rows * bins * bins, bytes_accessed=4 * bins * BLOCK, transcendentals=0
        ),
        name="filter_windows",
    )(offsets, steps, hi, lo, pieces)


def back_kernel(tiles_across, tiles_down, scale, off_ref, step_ref, w_ref, out_ref, f_ref, r_ref, g_ref, wt_ref, acc_ref):
    pairs, win, _ = w_ref.shape
    angles = 2 * pairs
    half = tiles_down // 2
    margin = STEP_MAX * half
    depth = angles * BAND
    j = pl.program_id(0)

    @pl.when(j == 0)
    def _():
        lane = lax.broadcasted_iota(jnp.int32, (win, LANES), 1)
        low = lane < LANES // 2
        for p in range(pairs):
            whole = w_ref[p].astype(jnp.float32)
            f_ref[margin : margin + win, :] = whole
            r_ref[margin : margin + win, :] = pltpu.roll(whole, LANES // 2, 1)
            jump = [margin + step_ref[2 * p + k, 1] * half for k in range(2)]
            g_ref[2 * p] = jnp.where(low, f_ref[margin : margin + win, :], r_ref[pl.ds(jump[0], win), :])
            g_ref[2 * p + 1] = jnp.where(low, r_ref[margin : margin + win, :], f_ref[pl.ds(jump[1], win), :])
        col = lax.broadcasted_iota(jnp.int32, (1, depth), 1)
        u_row = jnp.zeros((1, depth), jnp.int32)
        v_row = jnp.zeros((1, depth), jnp.int32)
        c_row = jnp.zeros((1, depth), jnp.int32)
        for a in range(angles):
            mine = (col >= a * BAND) & (col < (a + 1) * BAND)
            u, v = step_ref[a, 0], step_ref[a, 1]
            lead = off_ref[a] - TILE * tile_floor(off_ref[a], u, v)
            u_row = jnp.where(mine, u, u_row)
            v_row = jnp.where(mine, v, v_row)
            c_row = jnp.where(mine, lead - TILE * (col - a * BAND), c_row)
        across = lax.broadcasted_iota(jnp.int32, (TILE, depth), 0)
        line = (u_row * across + c_row).astype(jnp.float32)
        v_line = v_row.astype(jnp.float32)
        for y in range(TILE):
            away = jnp.abs(line + v_line * float(y)) * (1.0 / TILE)
            wt_ref[y * TILE : (y + 1) * TILE, :] = jnp.maximum(1.0 - away, 0.0).astype(jnp.bfloat16)

    base = []
    for a in range(angles):
        u, v = step_ref[a, 0], step_ref[a, 1]
        base.append(v * j - low_corner(u, v, tiles_across, tiles_down))

    def two_tiles(ii, carry):
        sides = []
        for e in range(2):
            bands = []
            for a in range(angles):
                start = base[a] + step_ref[a, 0] * (2 * ii + e)
                bands.append(g_ref[a, pl.ds(start, BAND), :].astype(jnp.bfloat16))
            sides.append(jnp.concatenate(bands, axis=0))
        bands = jnp.concatenate(sides, axis=1)
        tile = jnp.dot(wt_ref[...], bands, preferred_element_type=jnp.float32)
        tile = (tile * scale).astype(jnp.bfloat16)
        for e in range(2):
            for y in range(TILE):
                acc_ref[y, pl.ds(pl.multiple_of((2 * ii + e) * TILE, TILE), TILE), :] = tile[
                    y * TILE : (y + 1) * TILE, e * LANES : (e + 1) * LANES
                ]
        return carry

    lax.fori_loop(0, tiles_across // 2, two_tiles, 0, unroll=2)
    slices = LANES // 2
    for y in range(TILE):
        for part in range(tiles_across * TILE // LANES):
            cols = slice(part * LANES, (part + 1) * LANES)
            turned = acc_ref[y, cols, :].T
            out_ref[0, 0, y, :, cols] = turned[0:slices]
            out_ref[1, 0, y, :, cols] = turned[slices:]


def back_project(windows, offsets, steps, tiles_across, tiles_down):
    pairs, win, _ = windows.shape
    angles = 2 * pairs
    half = tiles_down // 2
    cols = tiles_across * TILE
    slices = LANES // 2
    margin = STEP_MAX * half
    smem = pl.BlockSpec(memory_space=pltpu.SMEM)
    scale = 2.0 / math.sqrt(angles)
    out = pl.pallas_call(
        functools.partial(back_kernel, tiles_across, tiles_down, scale),
        grid=(half,),
        in_specs=[smem, smem, pl.BlockSpec(memory_space=pltpu.VMEM)],
        out_specs=pl.BlockSpec((2, 1, TILE, slices, cols), lambda j: (0, j, 0, 0, 0)),
        out_shape=jax.ShapeDtypeStruct((2, half, TILE, slices, cols), jnp.bfloat16),
        scratch_shapes=[
            pltpu.VMEM((win + 2 * margin, LANES), jnp.float32),
            pltpu.VMEM((win + 2 * margin, LANES), jnp.float32),
            pltpu.VMEM((angles, win, LANES), jnp.float32),
            pltpu.VMEM((TILE * TILE, angles * BAND), jnp.bfloat16),
            pltpu.VMEM((TILE, cols, LANES), jnp.bfloat16),
        ],
        compiler_params=pltpu.CompilerParams(vmem_limit_bytes=40 * 1024 * 1024),
        cost_estimate=pl.CostEstimate(
            flops=2 * half * cols * TILE * LANES * angles * BAND, bytes_accessed=4 * half * TILE * slices * cols, transcendentals=0
        ),
        name="back_project",
    )(offsets, steps, windows)
    return out.reshape(tiles_down * TILE, slices, cols)


def shards(sinogram, offsets, steps):
    ang_count = lax.axis_size("ang")
    img_count = lax.axis_size("img")
    tiles_across = IMG // img_count // TILE
    tiles_down = IMG // ang_count // TILE
    angles_dev, slices, piece_bins = sinogram.shape
    pieces = lax.all_gather(sinogram.reshape(angles_dev * slices, piece_bins), "img", axis=0)
    windows = filter_windows(pieces, offsets, steps, ang_count, tiles_across, tiles_down)
    windows = lax.all_to_all(windows, "ang", 0, 0, tiled=True)
    return back_project(windows, offsets, steps, tiles_across, tiles_down)


def solution(mesh):
    return jax.shard_map(
        shards,
        mesh=mesh,
        in_specs=(P("ang", None, "img"), P(), P()),
        out_specs=P("ang", None, "img"),
        check_vma=False,
    )
```

```python
import functools
import math

import jax
import jax.numpy as jnp
import numpy as np
from jax import lax
from jax.experimental import pallas as pl
from jax.experimental.pallas import tpu as pltpu
from jax.sharding import PartitionSpec as P

IMG = 1024
STEP_MAX = 32
TILE = 16
BLOCK = 256
LANES = 128
REACH = math.isqrt(2 * STEP_MAX * STEP_MAX)
BAND = -(-(((TILE - 1) * REACH + TILE - 1) // TILE + 2) // 16) * 16


def window_rows(tiles_across, tiles_down):
    far = math.isqrt(STEP_MAX**2 * ((tiles_across - 1) ** 2 + (tiles_down - 1) ** 2))
    return -(-(far + BAND) // 16) * 16


def tile_floor(off, u, v):
    return (off + (TILE - 1) * (jnp.minimum(u, 0) + jnp.minimum(v, 0))) >> 4


def low_corner(u, v, tiles_across, tiles_down):
    return jnp.minimum(u, 0) * (tiles_across - 1) + jnp.minimum(v, 0) * (tiles_down - 1)


def ramp_strips(bins):
    row = np.arange(2 * bins - LANES)[:, None]
    gap = np.arange(LANES)[None, :] - row + bins - LANES
    safe = np.where(gap == 0, 1, gap).astype(np.float64)
    value = np.where(gap % 2 != 0, -1.0 / (math.pi**2 * safe * safe), 0.0)
    value = np.where(gap == 0, 0.25, value).astype(np.float32)
    hi = value.astype(jnp.bfloat16)
    near = slice(bins - LANES - BLOCK - LANES, bins - LANES + 2 * BLOCK)
    lo = (value[near] - hi[near].astype(np.float32)).astype(jnp.bfloat16)
    return hi, lo


def strip_block(ref, start, depth):
    left = ref[pl.ds(pl.multiple_of(start, LANES), depth), :]
    right = ref[pl.ds(pl.multiple_of(start - LANES, LANES), depth), :]
    return jnp.concatenate([left, right], axis=1)


def early_kernel(early_index, bins, hi_ref, *refs):
    x_refs, part_ref = refs[:-1], refs[-1]
    piece_bins = x_refs[0].shape[1]
    index = early_index(lax.axis_index("img"))

    def one_block(kb, carry):
        total = None
        for q, x_ref in zip(index, x_refs):
            block = strip_block(hi_ref, bins - LANES - kb * BLOCK + q * piece_bins, piece_bins)
            term = jnp.dot(x_ref[...], block, preferred_element_type=jnp.float32)
            total = term if total is None else total + term
        part_ref[kb] = total
        return carry

    lax.fori_loop(0, bins // BLOCK, one_block, 0, unroll=4)


def late_kernel(early_index, late_index, late_source, targets, tiles_across, tiles_down, win, *refs):
    off_ref, step_ref, hi_ref, lo_ref, part_ref = refs[:5]
    xs_ref, ft_ref = refs[-2:]
    out_refs = refs[-2 - targets : -2]
    x_refs = refs[5 : -2 - targets]
    rows, piece_bins = x_refs[0].shape
    blocks = part_ref.shape[0]
    bins = blocks * BLOCK
    here = lax.axis_index("img")
    early, late = early_index(here), late_index(here)
    edge = jnp.zeros((rows, BLOCK), jnp.bfloat16)
    xs_ref[:, 0:BLOCK] = edge
    xs_ref[:, BLOCK + bins :] = edge

    def place(q, x_ref):
        xs_ref[:, pl.ds(pl.multiple_of(BLOCK + q * piece_bins, LANES), piece_bins)] = x_ref[...]

    for q, x_ref in zip(early, x_refs):
        place(q, x_ref)
    for q, choices in zip(late, late_source(here, x_refs[len(early) :])):
        for when, x_ref in choices:
            if when is None:
                place(q, x_ref)
            else:
                pl.when(when)(functools.partial(place, q, x_ref))
    ft_ref[bins:, :] = jnp.zeros((ft_ref.shape[0] - bins, LANES), jnp.float32)

    def one_block(kb, carry):
        first = pl.multiple_of(kb * BLOCK, BLOCK)
        total = part_ref[kb]
        for q in late:
            block = strip_block(hi_ref, bins - LANES - kb * BLOCK + q * piece_bins, piece_bins)
            x = xs_ref[:, pl.ds(pl.multiple_of(BLOCK + q * piece_bins, LANES), piece_bins)]
            total += jnp.dot(x, block, preferred_element_type=jnp.float32)
        total += jnp.dot(
            xs_ref[:, pl.ds(first, 3 * BLOCK)], strip_block(lo_ref, LANES, 3 * BLOCK), preferred_element_type=jnp.float32
        )
        for half in range(BLOCK // LANES):
            ft_ref[pl.ds(first + half * LANES, LANES), :] = total[:, half * LANES : (half + 1) * LANES].T
        return carry

    lax.fori_loop(0, blocks, one_block, 0, unroll=2)

    mine = lax.axis_index("ang")
    lane = lax.broadcasted_iota(jnp.int32, (win, LANES), 1)
    for slot, out_ref in enumerate(out_refs):
        target = (mine >> 1) ^ slot
        start = []
        for k in range(2):
            a = mine * 2 + k
            u, v = step_ref[a, 0], step_ref[a, 1]
            start.append(
                tile_floor(off_ref[a], u, v)
                + u * (here * tiles_across)
                + v * (target * 2 * tiles_down)
                + low_corner(u, v, tiles_across, 2 * tiles_down)
            )
        both = jnp.where(lane < LANES // 2, ft_ref[pl.ds(start[0], win), :], ft_ref[pl.ds(start[1], win), :])
        out_ref[...] = both.astype(jnp.bfloat16)


def gather_plan(block, count):
    if count == 4:
        far = lax.ppermute(block, "img", [(i, i ^ 2) for i in range(4)])
        near = lax.ppermute(block, "img", [(i, i ^ 1) for i in range(4)])
        middle = lax.ppermute(block, "img", [(1, 2), (2, 1)])
        ends = lax.ppermute(far, "img", [(2, 3), (1, 0)])

        def late_source(z, refs):
            inner = (z == 1) | (z == 2)
            return [[(None, refs[0])], [(inner, refs[1]), (jnp.logical_not(inner), refs[2])]]

        return [block, near], [far, middle, ends], lambda z: [z, z ^ 1], lambda z: [z ^ 2, z ^ 3], late_source
    hops = [lax.ppermute(block, "img", [(i, (i + k) % count) for i in range(count)]) for k in range(1, count)]
    source = lambda z, ks: [lax.rem(z + (count - k), count) for k in ks]
    half = count // 2
    return (
        [block] + hops[: half - 1],
        hops[half - 1 :],
        lambda z: source(z, range(half)),
        lambda z: source(z, range(half, count)),
        lambda z, refs: [[(None, ref)] for ref in refs],
    )


def filter_windows(block, offsets, steps, count, targets, tiles_across, tiles_down):
    rows, piece_bins = block.shape
    bins = count * piece_bins
    win = window_rows(tiles_across, 2 * tiles_down)
    hi, lo = (jnp.asarray(x) for x in ramp_strips(bins))
    early, late, early_index, late_index, late_source = gather_plan(block, count)
    vmem = pl.BlockSpec(memory_space=pltpu.VMEM)
    smem = pl.BlockSpec(memory_space=pltpu.SMEM)
    params = pltpu.CompilerParams(vmem_limit_bytes=24 * 1024 * 1024)
    part = pl.pallas_call(
        functools.partial(early_kernel, early_index, bins),
        in_specs=[vmem] * (1 + len(early)),
        out_specs=vmem,
        out_shape=jax.ShapeDtypeStruct((bins // BLOCK, rows, BLOCK), jnp.float32),
        compiler_params=params,
        cost_estimate=pl.CostEstimate(flops=rows * bins * bins, bytes_accessed=8 * bins * LANES, transcendentals=0),
        name="filter_early",
    )(hi, *early)
    return pl.pallas_call(
        functools.partial(late_kernel, early_index, late_index, late_source, targets, tiles_across, tiles_down, win),
        in_specs=[smem, smem] + [vmem] * (3 + len(early) + len(late)),
        out_specs=[vmem] * targets,
        out_shape=[jax.ShapeDtypeStruct((win, LANES), jnp.bfloat16)] * targets,
        scratch_shapes=[
            pltpu.VMEM((rows, bins + 2 * BLOCK), jnp.bfloat16),
            pltpu.VMEM((bins + win, LANES), jnp.float32),
        ],
        compiler_params=params,
        cost_estimate=pl.CostEstimate(flops=rows * bins * bins, bytes_accessed=8 * bins * LANES, transcendentals=0),
        name="filter_late",
    )(offsets, steps, hi, lo, part, *early, *late)


def back_kernel(tiles_across, tiles_down, scale, *refs):
    off_ref, step_ref = refs[:2]
    f_ref, r_ref, g_ref, wt_ref, acc_ref = refs[-5:]
    out_ref, other_ref = refs[-6], refs[-7]
    own_refs = refs[2:-7]
    chips = len(own_refs)
    whole_win = own_refs[0].shape[0]
    win = g_ref.shape[1]
    half = tiles_down // 2
    margin = STEP_MAX * half
    slots = g_ref.shape[0]
    depth = slots * BAND
    j = pl.program_id(0)
    mine = lax.axis_index("ang")
    core = mine & 1

    angle = []
    for side in range(2):
        for c in range(chips):
            pair = ((mine >> 1) ^ c) * 2 + (core ^ side)
            angle += [pair * 2, pair * 2 + 1]
    u = [step_ref[a, 0] for a in angle]
    v = [step_ref[a, 1] for a in angle]

    @pl.when(j == 0)
    def _():
        lane = lax.broadcasted_iota(jnp.int32, (win, LANES), 1)
        low = lane < LANES // 2
        for p in range(slots // 2):
            whole = own_refs[p][...] if p < chips else other_ref[p - chips]
            whole = whole.astype(jnp.float32)
            f_ref[margin : margin + whole_win, :] = whole
            r_ref[margin : margin + whole_win, :] = pltpu.roll(whole, LANES // 2, 1)
            for k, (near, far) in enumerate(((f_ref, r_ref), (r_ref, f_ref))):
                s = 2 * p + k
                start = (
                    margin
                    + v[s] * (core * tiles_down)
                    + low_corner(u[s], v[s], tiles_across, tiles_down)
                    - low_corner(u[s], v[s], tiles_across, 2 * tiles_down)
                )
                g_ref[s] = jnp.where(low, near[pl.ds(start, win), :], far[pl.ds(start + v[s] * half, win), :])
        col = lax.broadcasted_iota(jnp.int32, (1, depth), 1)
        u_row = jnp.zeros((1, depth), jnp.int32)
        v_row = jnp.zeros((1, depth), jnp.int32)
        c_row = jnp.zeros((1, depth), jnp.int32)
        for s in range(slots):
            mask = (col >= s * BAND) & (col < (s + 1) * BAND)
            off = off_ref[angle[s]]
            lead = off - TILE * tile_floor(off, u[s], v[s])
            u_row = jnp.where(mask, u[s], u_row)
            v_row = jnp.where(mask, v[s], v_row)
            c_row = jnp.where(mask, lead - TILE * (col - s * BAND), c_row)
        across = lax.broadcasted_iota(jnp.int32, (TILE, depth), 0)
        line = (u_row * across + c_row).astype(jnp.float32)
        v_line = v_row.astype(jnp.float32)
        for y in range(TILE):
            away = jnp.abs(line + v_line * float(y)) * (1.0 / TILE)
            wt_ref[y * TILE : (y + 1) * TILE, :] = jnp.maximum(1.0 - away, 0.0).astype(jnp.bfloat16)

    base = [v[s] * j - low_corner(u[s], v[s], tiles_across, tiles_down) for s in range(slots)]

    def two_tiles(ii, carry):
        sides = []
        for e in range(2):
            bands = []
            for s in range(slots):
                start = base[s] + u[s] * (2 * ii + e)
                bands.append(g_ref[s, pl.ds(start, BAND), :].astype(jnp.bfloat16))
            sides.append(jnp.concatenate(bands, axis=0))
        bands = jnp.concatenate(sides, axis=1)
        tile = jnp.dot(wt_ref[...], bands, preferred_element_type=jnp.float32)
        tile = (tile * scale).astype(jnp.bfloat16)
        for e in range(2):
            for y in range(TILE):
                acc_ref[y, pl.ds(pl.multiple_of((2 * ii + e) * TILE, TILE), TILE), :] = tile[
                    y * TILE : (y + 1) * TILE, e * LANES : (e + 1) * LANES
                ]
        return carry

    lax.fori_loop(0, tiles_across // 2, two_tiles, 0, unroll=2)
    slices = LANES // 2
    for y in range(TILE):
        for part in range(tiles_across * TILE // LANES):
            cols = slice(part * LANES, (part + 1) * LANES)
            turned = acc_ref[y, cols, :].T
            out_ref[0, 0, y, :, cols] = turned[0:slices]
            out_ref[1, 0, y, :, cols] = turned[slices:]


def back_project(own, other, offsets, steps, tiles_across, tiles_down):
    chips = len(own)
    slots = 4 * chips
    win = window_rows(tiles_across, tiles_down)
    half = tiles_down // 2
    cols = tiles_across * TILE
    slices = LANES // 2
    margin = STEP_MAX * half
    smem = pl.BlockSpec(memory_space=pltpu.SMEM)
    vmem = pl.BlockSpec(memory_space=pltpu.VMEM)
    scale = 2.0 / math.sqrt(slots)
    padded = own[0].shape[0] + 2 * margin + win
    out = pl.pallas_call(
        functools.partial(back_kernel, tiles_across, tiles_down, scale),
        grid=(half,),
        in_specs=[smem, smem] + [vmem] * (chips + 1),
        out_specs=pl.BlockSpec((2, 1, TILE, slices, cols), lambda j: (0, j, 0, 0, 0)),
        out_shape=jax.ShapeDtypeStruct((2, half, TILE, slices, cols), jnp.bfloat16),
        scratch_shapes=[
            pltpu.VMEM((padded, LANES), jnp.float32),
            pltpu.VMEM((padded, LANES), jnp.float32),
            pltpu.VMEM((slots, win, LANES), jnp.float32),
            pltpu.VMEM((TILE * TILE, slots * BAND), jnp.bfloat16),
            pltpu.VMEM((TILE, cols, LANES), jnp.bfloat16),
        ],
        compiler_params=pltpu.CompilerParams(vmem_limit_bytes=24 * 1024 * 1024),
        cost_estimate=pl.CostEstimate(
            flops=2 * half * cols * TILE * LANES * slots * BAND, bytes_accessed=4 * half * TILE * slices * cols, transcendentals=0
        ),
        name="back_project",
    )(offsets, steps, *own, other)
    return out.reshape(tiles_down * TILE, slices, cols)


def shards(sinogram, offsets, steps):
    ang_count = lax.axis_size("ang")
    img_count = lax.axis_size("img")
    tiles_across = IMG // img_count // TILE
    tiles_down = IMG // ang_count // TILE
    angles_dev, slices, piece_bins = sinogram.shape
    block = sinogram.reshape(angles_dev * slices, piece_bins)
    chips = ang_count // 2
    windows = filter_windows(block, offsets, steps, img_count, chips, tiles_across, tiles_down)
    own = [windows[0]]
    for slot in range(1, chips):
        own.append(lax.ppermute(windows[slot], "ang", [(i, i ^ (2 * slot)) for i in range(ang_count)]))
    other = lax.ppermute(jnp.stack(own), "ang", [(i, i ^ 1) for i in range(ang_count)])
    return back_project(own, other, offsets, steps, tiles_across, tiles_down)


def solution(mesh):
    return jax.shard_map(
        shards,
        mesh=mesh,
        in_specs=(P("ang", None, "img"), P(), P()),
        out_specs=P("ang", None, "img"),
        check_vma=False,
    )
```

```python
import functools
import math

import jax
import jax.numpy as jnp
import numpy as np
from jax import lax
from jax.experimental import pallas as pl
from jax.experimental.pallas import tpu as pltpu
from jax.sharding import PartitionSpec as P

IMG = 1024
STEP_MAX = 32
TILE = 16
BLOCK = 256
LANES = 128
REACH = math.isqrt(2 * STEP_MAX * STEP_MAX)
BAND = -(-(((TILE - 1) * REACH + TILE - 1) // TILE + 2) // 16) * 16


def window_rows(tiles_across, tiles_down):
    far = math.isqrt(STEP_MAX**2 * ((tiles_across - 1) ** 2 + (tiles_down - 1) ** 2))
    return -(-(far + BAND) // 16) * 16


def tile_floor(off, u, v):
    return (off + (TILE - 1) * (jnp.minimum(u, 0) + jnp.minimum(v, 0))) >> 4


def low_corner(u, v, tiles_across, tiles_down):
    return jnp.minimum(u, 0) * (tiles_across - 1) + jnp.minimum(v, 0) * (tiles_down - 1)


def ramp_strips(bins):
    row = np.arange(2 * bins - LANES)[:, None]
    gap = np.arange(LANES)[None, :] - row + bins - LANES
    safe = np.where(gap == 0, 1, gap).astype(np.float64)
    value = np.where(gap % 2 != 0, -1.0 / (math.pi**2 * safe * safe), 0.0)
    value = np.where(gap == 0, 0.25, value).astype(np.float32)
    hi = value.astype(jnp.bfloat16)
    near = slice(bins - 3 * LANES, bins - LANES + BLOCK + LANES)
    lo = (value[near] - hi[near].astype(np.float32)).astype(jnp.bfloat16)
    return hi, lo


def strip_block(ref, start, depth):
    left = ref[pl.ds(pl.multiple_of(start, LANES), depth), :]
    right = ref[pl.ds(pl.multiple_of(start - LANES, LANES), depth), :]
    return jnp.concatenate([left, right], axis=1)


def lanes_of(q, piece_bins):
    return pl.ds(pl.multiple_of(BLOCK + q * piece_bins, LANES), piece_bins)


def partial_kernel(index, bins, seeded, hi_ref, *refs):
    x_refs, part_ref = refs[seeded:-1], refs[-1]
    piece_bins = x_refs[0].shape[1]
    index = index(lax.axis_index("img"))

    def one_block(kb, carry):
        total = refs[0][kb] if seeded else None
        for q, x_ref in zip(index, x_refs):
            block = strip_block(hi_ref, bins - LANES - kb * BLOCK + q * piece_bins, piece_bins)
            term = jnp.dot(x_ref[...], block, preferred_element_type=jnp.float32)
            total = term if total is None else total + term
        part_ref[kb] = total
        return carry

    lax.fori_loop(0, bins // BLOCK, one_block, 0, unroll=4)


def late_kernel(plan, targets, tiles_across, tiles_down, win, *refs):
    off_ref, step_ref, hi_ref, lo_ref, part_ref = refs[:5]
    xs_ref, ft_ref = refs[-2:]
    out_refs = refs[-2 - targets : -2]
    x_refs = refs[5 : -2 - targets]
    rows, piece_bins = x_refs[0].shape
    blocks = part_ref.shape[0]
    bins = blocks * BLOCK
    here = lax.axis_index("img")
    edge = jnp.zeros((rows, BLOCK), jnp.bfloat16)
    xs_ref[:, 0:BLOCK] = edge
    xs_ref[:, BLOCK + bins :] = edge

    def place(q, x_ref):
        xs_ref[:, lanes_of(q, piece_bins)] = x_ref[...]

    for when, q, x_ref in plan(here, x_refs):
        if when is None:
            place(q, x_ref)
        else:
            pl.when(when)(functools.partial(place, q, x_ref))
    last = plan(here, x_refs)[-1][1]
    ft_ref[bins:, :] = jnp.zeros((ft_ref.shape[0] - bins, LANES), jnp.float32)

    def one_block(kb, carry):
        first = pl.multiple_of(kb * BLOCK, BLOCK)
        near = pl.ds(pl.multiple_of(first + BLOCK - LANES, LANES), BLOCK + 2 * LANES)
        total = part_ref[kb]
        block = strip_block(hi_ref, bins - LANES - kb * BLOCK + last * piece_bins, piece_bins)
        total += jnp.dot(xs_ref[:, lanes_of(last, piece_bins)], block, preferred_element_type=jnp.float32)
        total += jnp.dot(
            xs_ref[:, near], strip_block(lo_ref, LANES, BLOCK + 2 * LANES), preferred_element_type=jnp.float32
        )
        for half in range(BLOCK // LANES):
            ft_ref[pl.ds(first + half * LANES, LANES), :] = total[:, half * LANES : (half + 1) * LANES].T
        return carry

    lax.fori_loop(0, blocks, one_block, 0, unroll=4)

    mine = lax.axis_index("ang")
    chunk = 16
    low = lax.broadcasted_iota(jnp.int32, (chunk, LANES), 1) < LANES // 2
    for slot in reversed(range(targets)):
        target = (mine >> 1) ^ slot
        start = []
        for k in range(2):
            a = mine * 2 + k
            u, v = step_ref[0, a], step_ref[1, a]
            start.append(
                tile_floor(off_ref[a], u, v)
                + u * (here * tiles_across)
                + v * (target * 2 * tiles_down)
                + low_corner(u, v, tiles_across, 2 * tiles_down)
            )
        for r in range(0, win, chunk):
            first, second = (ft_ref[pl.ds(at + r, chunk), :] for at in start)
            out_refs[slot][r : r + chunk, :] = jnp.where(low, first, second).astype(jnp.bfloat16)


def filter_windows(block, offsets, steps, count, targets, tiles_across, tiles_down):
    rows, piece_bins = block.shape
    bins = count * piece_bins
    win = window_rows(tiles_across, 2 * tiles_down)
    hi, lo = (jnp.asarray(x) for x in ramp_strips(bins))
    vmem = pl.BlockSpec(memory_space=pltpu.VMEM)
    smem = pl.BlockSpec(memory_space=pltpu.SMEM)
    params = pltpu.CompilerParams(vmem_limit_bytes=20 * 1024 * 1024)

    def partial(index, pieces, part=None):
        seed = [] if part is None else [part]
        return pl.pallas_call(
            functools.partial(partial_kernel, index, bins, len(seed)),
            in_specs=[vmem] * (1 + len(seed) + len(pieces)),
            out_specs=vmem,
            out_shape=jax.ShapeDtypeStruct((bins // BLOCK, rows, BLOCK), jnp.float32),
            compiler_params=params,
            cost_estimate=pl.CostEstimate(
                flops=2 * rows * bins * piece_bins * len(pieces), bytes_accessed=8 * bins * LANES, transcendentals=0
            ),
            name="filter_part%d" % len(pieces),
        )(hi, *seed, *pieces)

    def send(x, pairs):
        return lax.ppermute(x, "img", pairs)

    if count == 4:
        far = send(block, [(i, i ^ 2) for i in range(4)])
        near = send(block, [(i, i ^ 1) for i in range(4)])
        part = partial(lambda z: [z, z ^ 1], [block, near])
        far, again, part = lax.optimization_barrier((far, block, part))
        ends = send(far, [(2, 3), (1, 0)])
        middle = send(again, [(1, 2), (2, 1)])
        part = partial(lambda z: [z ^ 2], [far], part)
        pieces = [block, near, far, middle, ends]

        def plan(z, refs):
            inner = (z == 1) | (z == 2)
            return [
                (None, z, refs[0]),
                (None, z ^ 1, refs[1]),
                (None, z ^ 2, refs[2]),
                (inner, z ^ 3, refs[3]),
                (jnp.logical_not(inner), z ^ 3, refs[4]),
            ]
    else:
        pieces = [block] + [send(block, [(i, (i + k) % count) for i in range(count)]) for k in range(1, count)]
        part = partial(lambda z: [lax.rem(z + (count - k), count) for k in range(count - 1)], pieces[:-1])

        def plan(z, refs):
            return [(None, lax.rem(z + (count - k), count), ref) for k, ref in enumerate(refs)]

    return pl.pallas_call(
        functools.partial(late_kernel, plan, targets, tiles_across, tiles_down, win),
        in_specs=[smem, smem] + [vmem] * (3 + len(pieces)),
        out_specs=[vmem] * targets,
        out_shape=[jax.ShapeDtypeStruct((win, LANES), jnp.bfloat16)] * targets,
        scratch_shapes=[
            pltpu.VMEM((rows, bins + 2 * BLOCK), jnp.bfloat16),
            pltpu.VMEM((bins + win, LANES), jnp.float32),
        ],
        compiler_params=params,
        cost_estimate=pl.CostEstimate(
            flops=3 * rows * bins * piece_bins, bytes_accessed=8 * bins * LANES, transcendentals=0
        ),
        name="filter_late",
    )(offsets, steps, hi, lo, part, *pieces)


def slot_angles(side, chips):
    mine = lax.axis_index("ang")
    angles = []
    for c in range(chips):
        pair = ((mine >> 1) ^ c) * 2 + ((mine & 1) ^ side)
        angles += [pair * 2, pair * 2 + 1]
    return angles


def spread(windows, angles, step_ref, tiles_across, tiles_down, win, g_ref, scratch):
    half = tiles_down // 2
    margin = STEP_MAX * half
    core = lax.axis_index("ang") & 1
    chunk = 16
    low = lax.broadcasted_iota(jnp.int32, (chunk, LANES), 1) < LANES // 2
    for p, window in enumerate(windows):
        f_ref, r_ref = scratch[2 * (p % 2) : 2 * (p % 2) + 2]
        for r in range(0, window.shape[0], chunk):
            rows = window[r : r + chunk, :].astype(jnp.float32)
            f_ref[margin + r : margin + r + chunk, :] = rows
            r_ref[margin + r : margin + r + chunk, :] = pltpu.roll(rows, LANES // 2, 1)
        for k, (near, far) in enumerate(((f_ref, r_ref), (r_ref, f_ref))):
            s = 2 * p + k
            u, v = step_ref[0, angles[s]], step_ref[1, angles[s]]
            start = (
                margin
                + v * (core * tiles_down)
                + low_corner(u, v, tiles_across, tiles_down)
                - low_corner(u, v, tiles_across, 2 * tiles_down)
            )
            for r in range(0, win, chunk):
                g_ref[s, r : r + chunk, :] = jnp.where(
                    low, near[pl.ds(start + r, chunk), :], far[pl.ds(start + v * half + r, chunk), :]
                )


def own_kernel(tiles_across, tiles_down, win, *refs):
    off_ref, step_ref = refs[:2]
    g_ref, wt_ref = refs[-6:-4]
    windows = refs[2:-6]
    chips = len(windows)
    own = slot_angles(0, chips)
    spread(windows, own, step_ref, tiles_across, tiles_down, win, g_ref, refs[-4:])
    angles = own + slot_angles(1, chips)
    depth = len(angles) * BAND
    col = lax.broadcasted_iota(jnp.int32, (1, depth), 1)
    u_row = jnp.zeros((1, depth), jnp.int32)
    v_row = jnp.zeros((1, depth), jnp.int32)
    c_row = jnp.zeros((1, depth), jnp.int32)
    for s, a in enumerate(angles):
        mask = (col >= s * BAND) & (col < (s + 1) * BAND)
        u, v, off = step_ref[0, a], step_ref[1, a], off_ref[a]
        lead = off - TILE * tile_floor(off, u, v)
        u_row = jnp.where(mask, u, u_row)
        v_row = jnp.where(mask, v, v_row)
        c_row = jnp.where(mask, lead - TILE * (col - s * BAND), c_row)
    across = lax.broadcasted_iota(jnp.int32, (TILE, depth), 0)
    line = (u_row * across + c_row).astype(jnp.float32)
    v_line = v_row.astype(jnp.float32)
    for y in range(TILE):
        away = jnp.abs(line + v_line * float(y)) * (1.0 / TILE)
        wt_ref[y * TILE : (y + 1) * TILE, :] = jnp.maximum(1.0 - away, 0.0).astype(jnp.bfloat16)


def back_kernel(tiles_across, tiles_down, scale, step_ref, other_ref, own_ref, wt_ref, out_ref, g_ref, *scratch):
    chips = other_ref.shape[0]
    win = g_ref.shape[1]
    half = tiles_down // 2
    acc_refs = scratch[-2:]
    step = pl.program_id(0)
    slices = LANES // 2
    angles = slot_angles(0, chips) + slot_angles(1, chips)
    slots = len(angles)

    @pl.when(step == 0)
    def _():
        windows = [other_ref.at[c] for c in range(chips)]
        spread(windows, angles[slots // 2 :], step_ref, tiles_across, tiles_down, win, g_ref, scratch[:4])

    def multiply(acc_ref):
        u = [step_ref[0, a] for a in angles]
        v = [step_ref[1, a] for a in angles]
        base = [v[s] * step - low_corner(u[s], v[s], tiles_across, tiles_down) for s in range(slots)]
        for first in range(0, tiles_across, 2):
            sides = []
            for i in (first, first + 1):
                bands = []
                for s in range(slots):
                    ref, row = (own_ref, s) if s < slots // 2 else (g_ref, s - slots // 2)
                    bands.append(ref[row, pl.ds(base[s] + u[s] * i, BAND), :].astype(jnp.bfloat16))
                sides.append(jnp.concatenate(bands, axis=0))
            bands = jnp.concatenate(sides, axis=1)
            tile = jnp.dot(wt_ref[...], bands, preferred_element_type=jnp.float32)
            tile = (tile * scale).astype(jnp.bfloat16)
            for e in range(2):
                for y in range(TILE):
                    acc_ref[y, (first + e) * TILE : (first + e + 1) * TILE, :] = tile[
                        y * TILE : (y + 1) * TILE, e * LANES : (e + 1) * LANES
                    ]

    def turn(acc_ref):
        for y in range(TILE):
            for part in range(tiles_across * TILE // LANES):
                cols = slice(part * LANES, (part + 1) * LANES)
                turned = acc_ref[y, cols, :].T
                out_ref[0, 0, y, :, cols] = turned[0:slices]
                out_ref[1, 0, y, :, cols] = turned[slices:]

    for parity in range(2):

        @pl.when((step < half) & (lax.rem(step, 2) == parity))
        def _(parity=parity):
            turn(acc_refs[1 - parity])
            multiply(acc_refs[parity])

    @pl.when(step == half)
    def _():
        turn(acc_refs[(half - 1) % 2])


def back_project(own, other, offsets, steps, tiles_across, tiles_down):
    chips = len(own)
    slots = 4 * chips
    win = window_rows(tiles_across, tiles_down)
    half = tiles_down // 2
    cols = tiles_across * TILE
    slices = LANES // 2
    smem = pl.BlockSpec(memory_space=pltpu.SMEM)
    vmem = pl.BlockSpec(memory_space=pltpu.VMEM)
    scale = 2.0 / math.sqrt(slots)
    padded = own[0].shape[0] + 2 * STEP_MAX * half + win
    spread_scratch = [pltpu.VMEM((padded, LANES), jnp.float32)] * 4
    half_spread = jax.ShapeDtypeStruct((slots // 2, win, LANES), jnp.float32)
    params = pltpu.CompilerParams(vmem_limit_bytes=20 * 1024 * 1024)
    own_spread, weights = pl.pallas_call(
        functools.partial(own_kernel, tiles_across, tiles_down, win),
        in_specs=[smem, smem] + [vmem] * chips,
        out_specs=[vmem, vmem],
        out_shape=[half_spread, jax.ShapeDtypeStruct((TILE * TILE, slots * BAND), jnp.bfloat16)],
        scratch_shapes=spread_scratch,
        compiler_params=params,
        cost_estimate=pl.CostEstimate(flops=10**9, bytes_accessed=4 * slots * win * LANES, transcendentals=0),
        name="spread_own",
    )(offsets, steps, *own)
    out = pl.pallas_call(
        functools.partial(back_kernel, tiles_across, tiles_down, scale),
        grid=(half + 1,),
        in_specs=[smem] + [vmem] * 3,
        out_specs=pl.BlockSpec((2, 1, TILE, slices, cols), lambda j: (0, jnp.maximum(j - 1, 0), 0, 0, 0)),
        out_shape=jax.ShapeDtypeStruct((2, half, TILE, slices, cols), jnp.bfloat16),
        scratch_shapes=[pltpu.VMEM(half_spread.shape, jnp.float32)]
        + spread_scratch
        + [pltpu.VMEM((TILE, cols, LANES), jnp.bfloat16)] * 2,
        compiler_params=params,
        cost_estimate=pl.CostEstimate(
            flops=2 * half * cols * TILE * LANES * slots * BAND, bytes_accessed=4 * half * TILE * slices * cols, transcendentals=0
        ),
        name="back_project",
    )(steps, other, own_spread, weights)
    return out.reshape(tiles_down * TILE, slices, cols)


def shards(sinogram, offsets, steps):
    ang_count = lax.axis_size("ang")
    img_count = lax.axis_size("img")
    tiles_across = IMG // img_count // TILE
    tiles_down = IMG // ang_count // TILE
    angles_dev, slices, piece_bins = sinogram.shape
    steps = steps.T
    block = sinogram.reshape(angles_dev * slices, piece_bins)
    chips = ang_count // 2
    windows = filter_windows(block, offsets, steps, img_count, chips, tiles_across, tiles_down)
    own = [windows[0]]
    for slot in range(1, chips):
        own.append(lax.ppermute(windows[slot], "ang", [(i, i ^ (2 * slot)) for i in range(ang_count)]))
    other = lax.ppermute(jnp.stack(own), "ang", [(i, i ^ 1) for i in range(ang_count)])
    return back_project(own, other, offsets, steps, tiles_across, tiles_down)


def solution(mesh):
    return jax.shard_map(
        shards,
        mesh=mesh,
        in_specs=(P("ang", None, "img"), P(), P()),
        out_specs=P("ang", None, "img"),
        check_vma=False,
    )
```

```python
import functools
import math

import jax
import jax.numpy as jnp
import numpy as np
from jax import lax
from jax.experimental import pallas as pl
from jax.experimental.pallas import tpu as pltpu
from jax.sharding import PartitionSpec as P

IMG = 1024
STEP_MAX = 32
TILE = 16
BLOCK = 256
LANES = 128
REACH = math.isqrt(2 * STEP_MAX * STEP_MAX)
BAND = -(-(((TILE - 1) * REACH + TILE - 1) // TILE + 2) // 16) * 16


def window_rows(tiles_across, tiles_down):
    far = math.isqrt(STEP_MAX**2 * ((tiles_across - 1) ** 2 + (tiles_down - 1) ** 2))
    return -(-(far + BAND) // 16) * 16


def tile_floor(off, u, v):
    return (off + (TILE - 1) * (jnp.minimum(u, 0) + jnp.minimum(v, 0))) >> 4


def low_corner(u, v, tiles_across, tiles_down):
    return jnp.minimum(u, 0) * (tiles_across - 1) + jnp.minimum(v, 0) * (tiles_down - 1)


def ramp_strips(bins):
    row = np.arange(2 * bins - LANES)[:, None]
    gap = np.arange(LANES)[None, :] - row + bins - LANES
    safe = np.where(gap == 0, 1, gap).astype(np.float64)
    value = np.where(gap % 2 != 0, -1.0 / (math.pi**2 * safe * safe), 0.0)
    value = np.where(gap == 0, 0.25, value).astype(np.float32)
    hi = value.astype(jnp.bfloat16)
    near = slice(bins - 3 * LANES, bins - LANES + BLOCK + LANES)
    lo = (value[near] - hi[near].astype(np.float32)).astype(jnp.bfloat16)
    return hi, lo


def strip_block(ref, start, depth):
    left = ref[pl.ds(pl.multiple_of(start, LANES), depth), :]
    right = ref[pl.ds(pl.multiple_of(start - LANES, LANES), depth), :]
    return jnp.concatenate([left, right], axis=1)


def lanes_of(q, piece_bins):
    return pl.ds(pl.multiple_of(BLOCK + q * piece_bins, LANES), piece_bins)


def partial_kernel(index, bins, seeded, hi_ref, *refs):
    x_refs, part_ref = refs[seeded:-1], refs[-1]
    piece_bins = x_refs[0].shape[1]
    index = index(lax.axis_index("img"))

    def one_block(kb, carry):
        total = refs[0][kb] if seeded else None
        for q, x_ref in zip(index, x_refs):
            block = strip_block(hi_ref, bins - LANES - kb * BLOCK + q * piece_bins, piece_bins)
            term = jnp.dot(x_ref[...], block, preferred_element_type=jnp.float32)
            total = term if total is None else total + term
        part_ref[kb] = total
        return carry

    lax.fori_loop(0, bins // BLOCK, one_block, 0, unroll=4)


def late_kernel(plan, targets, tiles_across, tiles_down, win, *refs):
    off_ref, step_ref, hi_ref, lo_ref, part_ref = refs[:5]
    xs_ref, ft_ref = refs[-2:]
    out_refs = refs[-2 - targets : -2]
    x_refs = refs[5 : -2 - targets]
    rows, piece_bins = x_refs[0].shape
    blocks = part_ref.shape[0]
    bins = blocks * BLOCK
    here = lax.axis_index("img")
    edge = jnp.zeros((rows, BLOCK), jnp.bfloat16)
    xs_ref[:, 0:BLOCK] = edge
    xs_ref[:, BLOCK + bins :] = edge

    def place(q, x_ref):
        xs_ref[:, lanes_of(q, piece_bins)] = x_ref[...]

    for when, q, x_ref in plan(here, x_refs):
        if when is None:
            place(q, x_ref)
        else:
            pl.when(when)(functools.partial(place, q, x_ref))
    last = plan(here, x_refs)[-1][1]
    ft_ref[bins:, :] = jnp.zeros((ft_ref.shape[0] - bins, LANES), jnp.float32)

    def one_block(kb, carry):
        first = pl.multiple_of(kb * BLOCK, BLOCK)
        near = pl.ds(pl.multiple_of(first + BLOCK - LANES, LANES), BLOCK + 2 * LANES)
        total = part_ref[kb]
        block = strip_block(hi_ref, bins - LANES - kb * BLOCK + last * piece_bins, piece_bins)
        total += jnp.dot(xs_ref[:, lanes_of(last, piece_bins)], block, preferred_element_type=jnp.float32)
        total += jnp.dot(
            xs_ref[:, near], strip_block(lo_ref, LANES, BLOCK + 2 * LANES), preferred_element_type=jnp.float32
        )
        for half in range(BLOCK // LANES):
            ft_ref[pl.ds(first + half * LANES, LANES), :] = total[:, half * LANES : (half + 1) * LANES].T
        return carry

    lax.fori_loop(0, blocks, one_block, 0, unroll=4)

    mine = lax.axis_index("ang")
    chunk = 16
    low = lax.broadcasted_iota(jnp.int32, (chunk, LANES), 1) < LANES // 2
    for slot in reversed(range(targets)):
        target = (mine >> 1) ^ slot
        start = []
        for k in range(2):
            a = mine * 2 + k
            u, v = step_ref[0, a], step_ref[1, a]
            start.append(
                tile_floor(off_ref[a], u, v)
                + u * (here * tiles_across)
                + v * (target * 2 * tiles_down)
                + low_corner(u, v, tiles_across, 2 * tiles_down)
            )
        for r in range(0, win, chunk):
            first, second = (ft_ref[pl.ds(at + r, chunk), :] for at in start)
            out_refs[slot][r : r + chunk, :] = jnp.where(low, first, second).astype(jnp.bfloat16)


def filter_windows(block, offsets, steps, count, targets, tiles_across, tiles_down):
    rows, piece_bins = block.shape
    bins = count * piece_bins
    win = window_rows(tiles_across, 2 * tiles_down)
    hi, lo = (jnp.asarray(x) for x in ramp_strips(bins))
    vmem = pl.BlockSpec(memory_space=pltpu.VMEM)
    smem = pl.BlockSpec(memory_space=pltpu.SMEM)
    params = pltpu.CompilerParams(vmem_limit_bytes=20 * 1024 * 1024)

    def partial(index, pieces, part=None):
        seed = [] if part is None else [part]
        return pl.pallas_call(
            functools.partial(partial_kernel, index, bins, len(seed)),
            in_specs=[vmem] * (1 + len(seed) + len(pieces)),
            out_specs=vmem,
            out_shape=jax.ShapeDtypeStruct((bins // BLOCK, rows, BLOCK), jnp.float32),
            compiler_params=params,
            cost_estimate=pl.CostEstimate(
                flops=2 * rows * bins * piece_bins * len(pieces), bytes_accessed=8 * bins * LANES, transcendentals=0
            ),
            name="filter_part%d" % len(pieces),
        )(hi, *seed, *pieces)

    def send(x, pairs):
        return lax.ppermute(x, "img", pairs)

    if count == 4:
        far = send(block, [(i, i ^ 2) for i in range(4)])
        near = send(block, [(i, i ^ 1) for i in range(4)])
        part = partial(lambda z: [z], [block])
        ends = send(far, [(2, 3), (1, 0)])
        again, part = lax.optimization_barrier((block, far, part))[::2]
        middle = send(again, [(1, 2), (2, 1)])
        part = partial(lambda z: [z ^ 1, z ^ 2], [near, far], part)
        pieces = [block, near, far, middle, ends]

        def plan(z, refs):
            inner = (z == 1) | (z == 2)
            return [
                (None, z, refs[0]),
                (None, z ^ 1, refs[1]),
                (None, z ^ 2, refs[2]),
                (inner, z ^ 3, refs[3]),
                (jnp.logical_not(inner), z ^ 3, refs[4]),
            ]
    else:
        pieces = [block] + [send(block, [(i, (i + k) % count) for i in range(count)]) for k in range(1, count)]
        part = partial(lambda z: [lax.rem(z + (count - k), count) for k in range(count - 1)], pieces[:-1])

        def plan(z, refs):
            return [(None, lax.rem(z + (count - k), count), ref) for k, ref in enumerate(refs)]

    return pl.pallas_call(
        functools.partial(late_kernel, plan, targets, tiles_across, tiles_down, win),
        in_specs=[smem, smem] + [vmem] * (3 + len(pieces)),
        out_specs=[vmem] * targets,
        out_shape=[jax.ShapeDtypeStruct((win, LANES), jnp.bfloat16)] * targets,
        scratch_shapes=[
            pltpu.VMEM((rows, bins + 2 * BLOCK), jnp.bfloat16),
            pltpu.VMEM((bins + win, LANES), jnp.float32),
        ],
        compiler_params=params,
        cost_estimate=pl.CostEstimate(
            flops=3 * rows * bins * piece_bins, bytes_accessed=8 * bins * LANES, transcendentals=0
        ),
        name="filter_late",
    )(offsets, steps, hi, lo, part, *pieces)


def slot_angles(side, chips):
    mine = lax.axis_index("ang")
    angles = []
    for c in range(chips):
        pair = ((mine >> 1) ^ c) * 2 + ((mine & 1) ^ side)
        angles += [pair * 2, pair * 2 + 1]
    return angles


def spread(windows, angles, step_ref, tiles_across, tiles_down, win, g_ref, scratch):
    half = tiles_down // 2
    margin = STEP_MAX * half
    core = lax.axis_index("ang") & 1
    chunk = 16
    low = lax.broadcasted_iota(jnp.int32, (chunk, LANES), 1) < LANES // 2
    for p, window in enumerate(windows):
        f_ref, r_ref = scratch[2 * (p % 2) : 2 * (p % 2) + 2]
        for r in range(0, window.shape[0], chunk):
            rows = window[r : r + chunk, :].astype(jnp.float32)
            f_ref[margin + r : margin + r + chunk, :] = rows
            r_ref[margin + r : margin + r + chunk, :] = pltpu.roll(rows, LANES // 2, 1)
        for k, (near, far) in enumerate(((f_ref, r_ref), (r_ref, f_ref))):
            s = 2 * p + k
            u, v = step_ref[0, angles[s]], step_ref[1, angles[s]]
            start = (
                margin
                + v * (core * tiles_down)
                + low_corner(u, v, tiles_across, tiles_down)
                - low_corner(u, v, tiles_across, 2 * tiles_down)
            )
            for r in range(0, win, chunk):
                g_ref[s, r : r + chunk, :] = jnp.where(
                    low, near[pl.ds(start + r, chunk), :], far[pl.ds(start + v * half + r, chunk), :]
                )


def own_kernel(tiles_across, tiles_down, win, *refs):
    off_ref, step_ref = refs[:2]
    g_ref, wt_ref = refs[-6:-4]
    windows = refs[2:-6]
    chips = len(windows)
    own = slot_angles(0, chips)
    spread(windows, own, step_ref, tiles_across, tiles_down, win, g_ref, refs[-4:])
    angles = own + slot_angles(1, chips)
    depth = len(angles) * BAND
    col = lax.broadcasted_iota(jnp.int32, (1, depth), 1)
    u_row = jnp.zeros((1, depth), jnp.int32)
    v_row = jnp.zeros((1, depth), jnp.int32)
    c_row = jnp.zeros((1, depth), jnp.int32)
    for s, a in enumerate(angles):
        mask = (col >= s * BAND) & (col < (s + 1) * BAND)
        u, v, off = step_ref[0, a], step_ref[1, a], off_ref[a]
        lead = off - TILE * tile_floor(off, u, v)
        u_row = jnp.where(mask, u, u_row)
        v_row = jnp.where(mask, v, v_row)
        c_row = jnp.where(mask, lead - TILE * (col - s * BAND), c_row)
    across = lax.broadcasted_iota(jnp.int32, (TILE, depth), 0)
    line = (u_row * across + c_row).astype(jnp.float32)
    v_line = v_row.astype(jnp.float32)
    for y in range(TILE):
        away = jnp.abs(line + v_line * float(y)) * (1.0 / TILE)
        wt_ref[y * TILE : (y + 1) * TILE, :] = jnp.maximum(1.0 - away, 0.0).astype(jnp.bfloat16)


def back_kernel(tiles_across, tiles_down, scale, step_ref, other_ref, own_ref, wt_ref, out_ref, g_ref, *scratch):
    chips = other_ref.shape[0]
    win = g_ref.shape[1]
    half = tiles_down // 2
    acc_refs = scratch[-2:]
    step = pl.program_id(0)
    slices = LANES // 2
    angles = slot_angles(0, chips) + slot_angles(1, chips)
    slots = len(angles)

    @pl.when(step == 0)
    def _():
        windows = [other_ref.at[c] for c in range(chips)]
        spread(windows, angles[slots // 2 :], step_ref, tiles_across, tiles_down, win, g_ref, scratch[:4])

    def multiply(acc_ref):
        u = [step_ref[0, a] for a in angles]
        v = [step_ref[1, a] for a in angles]
        base = [v[s] * step - low_corner(u[s], v[s], tiles_across, tiles_down) for s in range(slots)]
        for first in range(0, tiles_across, 2):
            sides = []
            for i in (first, first + 1):
                bands = []
                for s in range(slots):
                    ref, row = (own_ref, s) if s < slots // 2 else (g_ref, s - slots // 2)
                    bands.append(ref[row, pl.ds(base[s] + u[s] * i, BAND), :].astype(jnp.bfloat16))
                sides.append(jnp.concatenate(bands, axis=0))
            bands = jnp.concatenate(sides, axis=1)
            tile = jnp.dot(wt_ref[...], bands, preferred_element_type=jnp.float32)
            tile = (tile * scale).astype(jnp.bfloat16)
            for e in range(2):
                for y in range(TILE):
                    acc_ref[y, (first + e) * TILE : (first + e + 1) * TILE, :] = tile[
                        y * TILE : (y + 1) * TILE, e * LANES : (e + 1) * LANES
                    ]

    def turn(acc_ref):
        for y in range(TILE):
            for part in range(tiles_across * TILE // LANES):
                cols = slice(part * LANES, (part + 1) * LANES)
                turned = acc_ref[y, cols, :].T
                out_ref[0, 0, y, :, cols] = turned[0:slices]
                out_ref[1, 0, y, :, cols] = turned[slices:]

    for parity in range(2):

        @pl.when((step < half) & (lax.rem(step, 2) == parity))
        def _(parity=parity):
            turn(acc_refs[1 - parity])
            multiply(acc_refs[parity])

    @pl.when(step == half)
    def _():
        turn(acc_refs[(half - 1) % 2])


def back_project(own, other, offsets, steps, tiles_across, tiles_down):
    chips = len(own)
    slots = 4 * chips
    win = window_rows(tiles_across, tiles_down)
    half = tiles_down // 2
    cols = tiles_across * TILE
    slices = LANES // 2
    smem = pl.BlockSpec(memory_space=pltpu.SMEM)
    vmem = pl.BlockSpec(memory_space=pltpu.VMEM)
    scale = 2.0 / math.sqrt(slots)
    padded = own[0].shape[0] + 2 * STEP_MAX * half + win
    spread_scratch = [pltpu.VMEM((padded, LANES), jnp.float32)] * 4
    half_spread = jax.ShapeDtypeStruct((slots // 2, win, LANES), jnp.float32)
    params = pltpu.CompilerParams(vmem_limit_bytes=20 * 1024 * 1024)
    own_spread, weights = pl.pallas_call(
        functools.partial(own_kernel, tiles_across, tiles_down, win),
        in_specs=[smem, smem] + [vmem] * chips,
        out_specs=[vmem, vmem],
        out_shape=[half_spread, jax.ShapeDtypeStruct((TILE * TILE, slots * BAND), jnp.bfloat16)],
        scratch_shapes=spread_scratch,
        compiler_params=params,
        cost_estimate=pl.CostEstimate(flops=10**9, bytes_accessed=4 * slots * win * LANES, transcendentals=0),
        name="spread_own",
    )(offsets, steps, *own)
    out = pl.pallas_call(
        functools.partial(back_kernel, tiles_across, tiles_down, scale),
        grid=(half + 1,),
        in_specs=[smem] + [vmem] * 3,
        out_specs=pl.BlockSpec((2, 1, TILE, slices, cols), lambda j: (0, jnp.maximum(j - 1, 0), 0, 0, 0)),
        out_shape=jax.ShapeDtypeStruct((2, half, TILE, slices, cols), jnp.bfloat16),
        scratch_shapes=[pltpu.VMEM(half_spread.shape, jnp.float32)]
        + spread_scratch
        + [pltpu.VMEM((TILE, cols, LANES), jnp.bfloat16)] * 2,
        compiler_params=params,
        cost_estimate=pl.CostEstimate(
            flops=2 * half * cols * TILE * LANES * slots * BAND, bytes_accessed=4 * half * TILE * slices * cols, transcendentals=0
        ),
        name="back_project",
    )(steps, other, own_spread, weights)
    return out.reshape(tiles_down * TILE, slices, cols)


def shards(sinogram, offsets, steps):
    ang_count = lax.axis_size("ang")
    img_count = lax.axis_size("img")
    tiles_across = IMG // img_count // TILE
    tiles_down = IMG // ang_count // TILE
    angles_dev, slices, piece_bins = sinogram.shape
    steps = steps.T
    block = sinogram.reshape(angles_dev * slices, piece_bins)
    chips = ang_count // 2
    windows = filter_windows(block, offsets, steps, img_count, chips, tiles_across, tiles_down)
    own = [windows[0]]
    for slot in range(1, chips):
        own.append(lax.ppermute(windows[slot], "ang", [(i, i ^ (2 * slot)) for i in range(ang_count)]))
    other = lax.ppermute(jnp.stack(own), "ang", [(i, i ^ 1) for i in range(ang_count)])
    return back_project(own, other, offsets, steps, tiles_across, tiles_down)


def solution(mesh):
    return jax.shard_map(
        shards,
        mesh=mesh,
        in_specs=(P("ang", None, "img"), P(), P()),
        out_specs=P("ang", None, "img"),
        check_vma=False,
    )
```
